32 devices in a mesh: beam: 2 (over x), freq: 8 (over z, y), sub: 2 (over core).
Axes of the slice: x: 2, y: 2, z: 4, core: 2. Of those that a mesh axis runs over, the one named last changes fastest.
Arguments:
- spectrum: bfloat16 [64, 2097152], P('sub', ('beam', 'freq')), parts along dimension 1
- hit_mask: int32 [64, 16384], P('sub', ('beam', 'freq')), parts along dimension 1, may hold values from 0 to 1, as said below
- owner_map: int32 [2048], P(('beam', 'freq')), parts along dimension 0, may hold values from 0 to 1023, as said below
- median_bin: int32 [2048], P(('beam', 'freq')), parts along dimension 0, may hold values from 32 to 559
- mad_bin: int32 [2048], P(('beam', 'freq')), parts along dimension 0, may hold values from 4 to 15
Outputs:
- hit_snr: bfloat16 [8, 2, 2048, 128], P('freq', 'sub', 'beam'), parts along dimension 2
- hit_keys: int32 [8, 2, 2048], P('freq', 'sub', 'beam'), parts along dimension 2
- hit_excess: float32 [8, 2, 2048], P('freq', 'sub', 'beam'), parts along dimension 2
The draws below stay inside these ranges and needn't reach their ends.
There are 2 independent parts, one for each index of `beam`. The reference program is written for one: setup_inputs(seed, part) draws one part's arguments, and reference() takes and returns one part's arrays. A program takes and returns all parts, laid end to end along the dimension named above; each array names one. Nothing has to cross between parts.
Inputs may be any that keep to these rules, and one draw needn't show every extreme that they name: `hit_mask`: for each index of freq, each half of the drift rates and each owner, at most 128 hit blocks go from the first to the last; in every draw some owner gets exactly 128 from every index of freq and half. `owner_map`: A permutation of the slots 0 to 1023; the 128 coarse channels of one index of freq go 16 to each owner, and the slot of index f's coarse channel at each owner is f.
All inputs are finite; a program needn't handle non-finite values.
Results may differ from the reference program's by a relative error of at most 0.007.
Values may be sent and summed in bfloat16 or wider, within the bound.
A program may use at most 64 MiB of HBM per device.

```python
import jax
import jax.numpy as jnp
from jax import lax

CHANNELS = 1048576
COARSE_WIDTH = 1024
BLOCK = 128
CAP = 128
DR_DEV = 32
DRIFTS = 64
COARSE = 1024
BPC = 8
NBLK = 8192
CD = 128
Q = 16
LIST = 1024
N_FREQ = 8
N_SUB = 2


def joint_draw(key):
    freq_count = COARSE // CD
    base = jax.random.fold_in(key, 101)
    parts = jax.random.split(base, 7)
    source_keys = jax.random.split(parts[0], freq_count)
    shuffled = jax.vmap(lambda one: jax.random.permutation(one, CD))(source_keys).astype(jnp.int32)
    source = jnp.arange(freq_count, dtype=jnp.int32)[:, None]
    owner = shuffled % freq_count
    local = source * Q + shuffled // freq_count
    owner_map = (owner * CD + local).reshape(COARSE).astype(jnp.int32)
    true_bin = jax.random.randint(parts[1], (COARSE,), 32, 160, dtype=jnp.int32)
    mad = jax.random.randint(parts[2], (COARSE,), 4, 16, dtype=jnp.int32)
    stale = (jax.random.randint(parts[3], (COARSE,), 0, 16, dtype=jnp.int32) == 0).astype(jnp.int32)
    median = true_bin + 400 * stale
    hot = jax.random.randint(parts[6], (), 0, freq_count, dtype=jnp.int32)
    dest = owner.reshape(COARSE)
    level = jax.random.randint(parts[4], (COARSE,), 0, 5, dtype=jnp.int32)
    limit = jnp.where(dest == hot, 1024, 32 * jnp.power(2, level)).astype(jnp.int32)
    tickets = jax.random.randint(parts[5], (DRIFTS, COARSE, BPC), 0, 1024, dtype=jnp.int32)
    raw = (tickets < limit[None, :, None]).astype(jnp.int32)
    half = (jnp.arange(DRIFTS, dtype=jnp.int32) // DR_DEV)[:, None, None]
    sender = (jnp.arange(COARSE, dtype=jnp.int32) // CD)[None, :, None]
    group = (half * freq_count + sender) * freq_count + dest[None, :, None]
    group = jnp.broadcast_to(group, (DRIFTS, COARSE, BPC)).reshape(-1)
    flat = raw.reshape(-1)
    groups_total = DRIFTS // DR_DEV * freq_count * freq_count
    order = jnp.argsort(group, stable=True)
    ordered = flat[order]
    running = jnp.cumsum(ordered).astype(jnp.int32)
    counts = jax.ops.segment_sum(flat, group, num_segments=groups_total)
    starts = (jnp.cumsum(counts) - counts).astype(jnp.int32)
    rank = running - starts[group[order]]
    keep = ordered * (rank <= CAP).astype(jnp.int32)
    mask = jnp.zeros_like(flat).at[order].set(keep).reshape(DRIFTS, COARSE, BPC)
    return (owner_map, median, mad, mask, true_bin)


def draw_owner_map(key, part):
    return joint_draw(key)[0]


def draw_median_bin(key, part):
    return joint_draw(key)[1]


def draw_mad_bin(key, part):
    return joint_draw(key)[2]


def draw_hit_mask(key, part):
    return joint_draw(key)[3].reshape(DRIFTS, NBLK)


def draw_spectrum(key, part):
    owner_map, median, mad, mask, true_bin = joint_draw(key)
    noise_key = jax.random.fold_in(key, 202)
    tone_key = jax.random.fold_in(key, 303)
    deviation = 1.4826 * 0.0625 * mad.astype(jnp.float32)
    center = 0.0625 * true_bin.astype(jnp.float32)
    ramp = 0.6 * jnp.power(3.0, jnp.arange(DRIFTS, dtype=jnp.float32) / max(DRIFTS - 1, 1))
    noise = jax.random.normal(noise_key, (DRIFTS, COARSE, BPC, BLOCK), jnp.float32)
    tone_at = jax.random.randint(tone_key, (DRIFTS, COARSE, BPC), 0, BLOCK, dtype=jnp.int32)
    tone = (jnp.arange(BLOCK, dtype=jnp.int32)[None, None, None, :] == tone_at[..., None]).astype(jnp.float32)
    tone = tone * mask[..., None].astype(jnp.float32)
    scale = deviation[None, :, None, None] * ramp[:, None, None, None]
    power = center[None, :, None, None] + scale * noise + 8.0 * scale * tone
    return power.reshape(DRIFTS, CHANNELS).astype(jnp.bfloat16)


def setup_inputs(seed: int = 0, part: int = 0) -> dict:
    key_of = jax.random.split(jax.random.key(seed), 6)
    own_keys = jax.random.split(jax.random.fold_in(key_of[5], part), 6)
    return {
        "spectrum": draw_spectrum(jax.random.fold_in(jax.random.fold_in(key_of[5], part), 71), part),
        "hit_mask": draw_hit_mask(jax.random.fold_in(jax.random.fold_in(key_of[5], part), 71), part),
        "owner_map": draw_owner_map(jax.random.fold_in(jax.random.fold_in(key_of[5], part), 71), part),
        "median_bin": draw_median_bin(jax.random.fold_in(jax.random.fold_in(key_of[5], part), 71), part),
        "mad_bin": draw_mad_bin(jax.random.fold_in(jax.random.fold_in(key_of[5], part), 71), part),
    }


BIN_STEP = 0.0625
MAD_WIDTH = 5.0
MAD_SCALE = 1.4826
THRESH = 3.0

def reference(spectrum, hit_mask, owner_map, median_bin, mad_bin):
    per_coarse = COARSE_WIDTH // BLOCK
    power = spectrum.astype(jnp.float32).reshape(DRIFTS, COARSE, COARSE_WIDTH)
    center = BIN_STEP * median_bin.astype(jnp.float32)
    spread = MAD_WIDTH * BIN_STEP * mad_bin.astype(jnp.float32)
    inside = (power >= (center - spread)[None, :, None]) & (power <= (center + spread)[None, :, None])
    kept = jnp.where(inside, power - center[None, :, None], jnp.float32(0.0))
    count = lax.optimization_barrier(jnp.sum(inside.astype(jnp.float32), axis=(0, 2)))
    first = lax.optimization_barrier(jnp.sum(kept, axis=(0, 2)))
    second = lax.optimization_barrier(jnp.sum(kept * kept, axis=(0, 2)))
    floor_count = jnp.maximum(count, 1.0)
    mean_level = center + first / floor_count
    mad_sigma = MAD_SCALE * BIN_STEP * mad_bin.astype(jnp.float32)
    sigma = jnp.sqrt(0.5 * second / floor_count + 0.5 * mad_sigma * mad_sigma)
    snr = ((power - mean_level[None, :, None]) / sigma[None, :, None]).astype(jnp.bfloat16)
    snr = snr.reshape(DRIFTS, COARSE, per_coarse, BLOCK)
    inverse = jnp.zeros((COARSE,), jnp.int32).at[owner_map].set(jnp.arange(COARSE, dtype=jnp.int32))
    by_slot = snr[:, inverse]
    marks = hit_mask.reshape(DRIFTS, COARSE, per_coarse)[:, inverse]
    by_slot = by_slot.reshape(N_SUB, DR_DEV, N_FREQ, CD, per_coarse, BLOCK).transpose(2, 0, 3, 1, 4, 5)
    by_slot = by_slot.reshape(N_FREQ * N_SUB, CD * DR_DEV * per_coarse, BLOCK)
    marks = marks.reshape(N_SUB, DR_DEV, N_FREQ, CD, per_coarse).transpose(2, 0, 3, 1, 4)
    marks = marks.reshape(N_FREQ * N_SUB, CD * DR_DEV * per_coarse).astype(jnp.int32)
    slots = jnp.arange(CD, dtype=jnp.int32)[None, None, :, None, None]
    halves = jnp.arange(N_SUB, dtype=jnp.int32)[None, :, None, None, None]
    drifts = jnp.arange(DR_DEV, dtype=jnp.int32)[None, None, None, :, None]
    blocks = jnp.arange(per_coarse, dtype=jnp.int32)[None, None, None, None, :]
    keys = (slots * DRIFTS + halves * DR_DEV + drifts) * per_coarse + blocks
    keys = jnp.broadcast_to(keys, (N_FREQ, N_SUB, CD, DR_DEV, per_coarse)).reshape(N_FREQ * N_SUB, -1)
    place = jnp.where(marks > 0, jnp.cumsum(marks, axis=-1).astype(jnp.int32) - 1, LIST).astype(jnp.int32)

    def collect(items):
        rows, key_row, place_row = items
        snr_list = jnp.zeros((LIST, BLOCK), jnp.bfloat16).at[place_row].set(rows, mode='drop')
        key_list = jnp.full((LIST,), -1, jnp.int32).at[place_row].set(key_row, mode='drop')
        excess = lax.optimization_barrier(jnp.sum(jnp.maximum(snr_list.astype(jnp.float32) - THRESH, 0.0), axis=-1))
        return (snr_list, key_list, excess)
    snr_lists, key_lists, excess = lax.map(collect, (by_slot, keys, place))
    return (snr_lists.reshape(N_FREQ, N_SUB, LIST, BLOCK), key_lists.reshape(N_FREQ, N_SUB, LIST), excess.reshape(N_FREQ, N_SUB, LIST))
```

```python
import functools

import jax
import jax.numpy as jnp
from jax import lax
from jax.experimental import pallas as pl
from jax.experimental.pallas import tpu as pltpu
from jax.sharding import PartitionSpec as P

COARSE_WIDTH = 1024
BLOCK = 128
CAP = 128
PER = COARSE_WIDTH // BLOCK

BIN_STEP = 0.0625
MAD_WIDTH = 5.0
MAD_SCALE = 1.4826
THRESH = 3.0

F32 = jnp.float32
BF16 = jnp.bfloat16
MESH = pl.DeviceIdType.MESH
NT = (((1,), (1,)), ((), ()))


def iota(shape, dim):
    return lax.broadcasted_iota(jnp.int32, shape, dim)


def one(mask, dtype=BF16):
    return jnp.where(mask, jnp.ones((), dtype), jnp.zeros((), dtype))


def positions(om_ref, mask_ref, turned, place):
    drifts = mask_ref.shape[0]
    coarse = place.shape[0]
    keys = PER * drifts
    turned[...] = mask_ref[...].astype(F32).T
    marks = jnp.concatenate([turned[pl.ds(b, coarse, stride=PER), :] for b in range(PER)], axis=1)
    rank_a = iota((keys, keys), 0)
    rank_b = iota((keys, keys), 1)
    rank_a = (rank_a % drifts) * PER + rank_a // drifts
    rank_b = (rank_b % drifts) * PER + rank_b // drifts
    before = jnp.dot(marks.astype(BF16), one(rank_a < rank_b), preferred_element_type=F32)
    count = jnp.sum(marks, axis=1, keepdims=True)
    wide = jnp.broadcast_to(om_ref[...], (coarse, coarse))
    eye = iota((coarse, coarse), 0) == iota((coarse, coarse), 1)
    tall = jnp.sum(jnp.where(eye, wide, 0), axis=1, keepdims=True)
    ahead = (wide // coarse == tall // coarse) & (wide < tall)
    offset = jnp.dot(
        one(ahead),
        jnp.broadcast_to(count, (coarse, keys)).astype(BF16),
        preferred_element_type=F32,
    )
    place[...] = jnp.where(marks > 0, offset + before, -1.0)


def local_kernel(
    om_s, med_s, mad_s, om_ref, mask_ref, spec_ref, rows_ref, tags_ref, mom_ref,
    turned, place, held, tagged, sums,
):
    step = pl.program_id(0)
    drifts = spec_ref.shape[0]
    coarse = place.shape[0]
    keys = PER * drifts
    chunk = spec_ref.shape[1] // COARSE_WIDTH

    @pl.when(step == 0)
    def _():
        positions(om_ref, mask_ref, turned, place)
        held[...] = jnp.zeros_like(held)
        tagged[...] = jnp.zeros_like(tagged)

    spot = iota((CAP, keys), 0).astype(F32).astype(BF16)
    lane = iota((8, keys), 1)
    row = iota((8, keys), 0)
    order = ((lane % drifts) * PER + lane // drifts).astype(F32)
    for k in range(chunk):
        c = step * chunk + k
        center = BIN_STEP * med_s[c].astype(F32)
        spread = MAD_WIDTH * BIN_STEP * mad_s[c].astype(F32)
        low, high = center - spread, center + spread
        total = [jnp.zeros((8, BLOCK), F32) for _ in range(3)]
        tiles = []
        for b in range(PER):
            tile = spec_ref[:, k * COARSE_WIDTH + b * BLOCK : k * COARSE_WIDTH + (b + 1) * BLOCK]
            tiles.append(tile)
            x = tile.astype(F32)
            inside = (x >= low) & (x <= high)
            kept = jnp.where(inside, x - center, 0.0)
            for i, v in enumerate((one(inside, F32), kept, kept * kept)):
                for r in range(0, drifts, 8):
                    total[i] = total[i] + v[r : r + 8]
        for i in range(3):
            sums[i, pl.ds(c, 1), :] = jnp.sum(total[i], axis=0, keepdims=True)
        line = jnp.broadcast_to(place[pl.ds(c, 1), :], (16, keys)).astype(BF16)
        pick = one(jnp.concatenate([line] * (CAP // 16), axis=0) == spot)
        dest = om_s[c] // coarse
        slot = (om_s[c] % coarse).astype(F32)
        held[dest] += jnp.dot(pick, jnp.concatenate(tiles, axis=0), preferred_element_type=F32)
        tag = jnp.where(
            row == 0, order, jnp.where(row == 1, slot, jnp.where(row == 2, c.astype(F32), 1.0))
        ).astype(BF16)
        tagged[dest] += lax.dot_general(tag, pick, NT, preferred_element_type=F32)

    @pl.when(step == pl.num_programs(0) - 1)
    def _():
        rows_ref[...] = held[...].astype(BF16)
        tags_ref[...] = tagged[...]
        flat = [jnp.sum(sums[i].T, axis=0, keepdims=True) for i in range(3)]
        mom_ref[...] = jnp.concatenate(flat + [jnp.zeros((5, coarse), F32)], axis=0)


def split3(v):
    a = v.astype(BF16).astype(F32)
    b = (v - a).astype(BF16).astype(F32)
    return [a, b, v - a - b]


def exchange_kernel(
    freq_count, drift_total, rows_ref, tags_ref, mom_ref, med_ref, mad_ref, snr_ref, keys_ref, excess_ref,
    other, rows_out, keys_out, rows_in, keys_in, mom_sem, row_send, row_recv, key_send, key_recv,
):
    me = lax.axis_index("freq")
    half = lax.axis_index("sub")
    coarse = mom_ref.shape[1]
    barrier = pltpu.get_barrier_semaphore()
    pl.semaphore_signal(barrier, inc=1, device_id={"sub": 1 - half}, device_id_type=MESH)
    for d in range(1, freq_count):
        pl.semaphore_signal(
            barrier, inc=1, device_id={"freq": lax.rem(me + d, freq_count)}, device_id_type=MESH
        )
    pl.semaphore_wait(barrier, freq_count)

    swap = pltpu.make_async_remote_copy(
        src_ref=mom_ref, dst_ref=other, send_sem=mom_sem.at[0], recv_sem=mom_sem.at[1],
        device_id={"sub": 1 - half}, device_id_type=MESH,
    )
    swap.start()
    swap.wait()
    moments = mom_ref[...] + other[...]
    floor_count = jnp.maximum(moments[0:1], 1.0)
    mad = mad_ref[...].astype(F32)
    mean_level = BIN_STEP * med_ref[...].astype(F32) + moments[1:2] / floor_count
    mad_sigma = MAD_SCALE * BIN_STEP * mad
    sigma = jnp.sqrt(0.5 * moments[2:3] / floor_count + 0.5 * mad_sigma * mad_sigma)
    table = jnp.concatenate(
        split3(mean_level) + split3(1.0 / sigma) + [jnp.zeros((2, coarse), F32)], axis=0
    ).astype(BF16)
    drift_dev = drift_total // lax.axis_size("sub")
    base = (half * (drift_dev * PER)).astype(F32)

    def prepare(o):
        tags = tags_ref[o]
        filled = tags[3:4] > 0.5
        hot = one((iota((coarse, CAP), 0).astype(F32) == tags[2:3]) & filled)
        vals = jnp.dot(table, hot, preferred_element_type=F32)
        level = vals[0:1] + vals[1:2] + vals[2:3]
        scale = vals[3:4] + vals[4:5] + vals[5:6]
        cols = jnp.concatenate([level, scale, jnp.zeros((6, CAP), F32)], axis=0).T
        rows_out[o] = ((rows_ref[o].astype(F32) - cols[:, 0:1]) * cols[:, 1:2]).astype(BF16)
        key = tags[1:2] * float(drift_total * PER) + base + tags[0:1]
        key = jnp.where(filled, key, -1.0).astype(jnp.int32)
        keys_out[o] = jnp.broadcast_to(key, (8, CAP))

    def send(d):
        to = lax.rem(me + d, freq_count)
        move = functools.partial(
            pltpu.make_async_remote_copy, device_id={"freq": to}, device_id_type=MESH
        )
        return (
            move(src_ref=rows_out.at[to], dst_ref=rows_in.at[me], send_sem=row_send.at[d], recv_sem=row_recv.at[d]),
            move(src_ref=keys_out.at[to], dst_ref=keys_in.at[me], send_sem=key_send.at[d], recv_sem=key_recv.at[d]),
        )

    for d in range(freq_count):
        prepare(lax.rem(me + d, freq_count))
    for d in range(1, freq_count):
        for copy in send(d):
            copy.start()
    rows_in[me] = rows_out[me]
    keys_in[me] = keys_out[me]
    for d in range(1, freq_count):
        for copy in send(d):
            copy.wait()

    begin = jnp.zeros((1, 1), F32)
    dst, key_row = [], []
    lanes = iota((1, CAP), 1).astype(F32)
    for f in range(freq_count):
        key = keys_in[f][0:1]
        live = key >= 0
        dst.append(jnp.where(live, begin + lanes, -1.0))
        key_row.append(key)
        begin = begin + jnp.sum(one(live, F32), axis=1, keepdims=True)
    dst = jnp.concatenate(dst, axis=1)
    key_row = jnp.concatenate(key_row, axis=1)
    width = freq_count * CAP
    digits = jnp.concatenate(
        [
            (key_row // 256).astype(F32),
            (key_row % 256).astype(F32),
            jnp.ones((1, width), F32),
            jnp.zeros((5, width), F32),
        ],
        axis=0,
    ).astype(BF16)
    spot = iota((CAP, width), 0).astype(F32).astype(BF16)
    arrived = rows_in[...].reshape(width, BLOCK)
    for k in range(freq_count):
        local = jnp.clip(dst - float(k * CAP), -1.0, float(CAP))
        line = jnp.broadcast_to(local, (16, width)).astype(BF16)
        pick = one(jnp.concatenate([line] * (CAP // 16), axis=0) == spot)
        out = jnp.dot(pick, arrived, preferred_element_type=F32)
        snr_ref[k * CAP : (k + 1) * CAP, :] = out.astype(BF16)
        got = lax.dot_general(digits, pick, NT, preferred_element_type=F32)
        key = jnp.where(got[2:3] > 0.5, got[0:1] * 256.0 + got[1:2], -1.0)
        keys_ref[:, k * CAP : (k + 1) * CAP] = key.astype(jnp.int32)
        over = jnp.maximum(out - THRESH, 0.0)
        excess_ref[:, k * CAP : (k + 1) * CAP] = jnp.sum(over.T, axis=0, keepdims=True)


def per_device(spectrum, hit_mask, owner_map, median_bin, mad_bin):
    drift_dev = spectrum.shape[0]
    coarse = owner_map.shape[0]
    freq_count = lax.axis_size("freq")
    drift_total = drift_dev * lax.axis_size("sub")
    width = freq_count * CAP
    chunk = 8
    smem = pl.BlockSpec(memory_space=pltpu.SMEM)
    vmem = pl.BlockSpec(memory_space=pltpu.VMEM)
    whole = lambda shape: pl.BlockSpec(shape, lambda i: (0,) * len(shape))
    rows, tags, moments = pl.pallas_call(
        local_kernel,
        grid=(coarse // chunk,),
        out_shape=(
            jax.ShapeDtypeStruct((freq_count, CAP, BLOCK), BF16),
            jax.ShapeDtypeStruct((freq_count, 8, CAP), F32),
            jax.ShapeDtypeStruct((8, coarse), F32),
        ),
        in_specs=[
            smem, smem, smem,
            whole((1, coarse)),
            whole((drift_dev, coarse * PER)),
            pl.BlockSpec((drift_dev, chunk * COARSE_WIDTH), lambda i: (0, i)),
        ],
        out_specs=(
            whole((freq_count, CAP, BLOCK)), whole((freq_count, 8, CAP)), whole((8, coarse))
        ),
        scratch_shapes=[
            pltpu.VMEM((coarse * PER, drift_dev), F32),
            pltpu.VMEM((coarse, PER * drift_dev), F32),
            pltpu.VMEM((freq_count, CAP, BLOCK), F32),
            pltpu.VMEM((freq_count, 8, CAP), F32),
            pltpu.VMEM((3, coarse, BLOCK), F32),
        ],
        compiler_params=pltpu.CompilerParams(dimension_semantics=("arbitrary",)),
        name="moments_and_pick",
    )(owner_map, median_bin, mad_bin, owner_map.reshape(1, coarse), hit_mask, spectrum)
    snr, keys, excess = pl.pallas_call(
        functools.partial(exchange_kernel, freq_count, drift_total),
        out_shape=(
            jax.ShapeDtypeStruct((width, BLOCK), BF16),
            jax.ShapeDtypeStruct((1, width), jnp.int32),
            jax.ShapeDtypeStruct((1, width), F32),
        ),
        in_specs=[vmem] * 5,
        out_specs=(vmem,) * 3,
        scratch_shapes=[
            pltpu.VMEM((8, coarse), F32),
            pltpu.VMEM((freq_count, CAP, BLOCK), BF16),
            pltpu.VMEM((freq_count, 8, CAP), jnp.int32),
            pltpu.VMEM((freq_count, CAP, BLOCK), BF16),
            pltpu.VMEM((freq_count, 8, CAP), jnp.int32),
            pltpu.SemaphoreType.DMA((2,)),
            pltpu.SemaphoreType.DMA((freq_count,)),
            pltpu.SemaphoreType.DMA((freq_count,)),
            pltpu.SemaphoreType.DMA((freq_count,)),
            pltpu.SemaphoreType.DMA((freq_count,)),
        ],
        compiler_params=pltpu.CompilerParams(collective_id=0, has_side_effects=True),
        name="exchange_and_list",
    )(rows, tags, moments, median_bin.reshape(1, coarse), mad_bin.reshape(1, coarse))
    return (
        snr.reshape(1, 1, width, BLOCK),
        keys.reshape(1, 1, width),
        excess.reshape(1, 1, width),
    )


def solution(mesh):
    placed = (
        P("sub", ("beam", "freq")),
        P("sub", ("beam", "freq")),
        P(("beam", "freq")),
        P(("beam", "freq")),
        P(("beam", "freq")),
    )
    return jax.shard_map(
        per_device,
        mesh=mesh,
        in_specs=placed,
        out_specs=(
            P("freq", "sub", "beam", None),
            P("freq", "sub", "beam"),
            P("freq", "sub", "beam"),
        ),
        check_vma=False,
    )
```

```python
import functools

import jax
import jax.numpy as jnp
from jax import lax
from jax.experimental import pallas as pl
from jax.experimental.pallas import tpu as pltpu
from jax.sharding import PartitionSpec as P

COARSE_WIDTH = 1024
BLOCK = 128
CAP = 128
PER = COARSE_WIDTH // BLOCK

BIN_STEP = 0.0625
MAD_WIDTH = 5.0
MAD_SCALE = 1.4826
THRESH = 3.0

F32 = jnp.float32
BF16 = jnp.bfloat16
MESH = pl.DeviceIdType.MESH
NT = (((1,), (1,)), ((), ()))
UNROLL = 8
OUT_SPEC = pl.BlockSpec(memory_space=pl.ANY)


def iota(shape, dim):
    return lax.broadcasted_iota(jnp.int32, shape, dim)


def one(mask, dtype=BF16):
    return jnp.where(mask, jnp.ones((), dtype), jnp.zeros((), dtype))


def split3(v):
    a = v.astype(BF16).astype(F32)
    b = (v - a).astype(BF16).astype(F32)
    return [a, b, v - a - b]


def plan(om_ref, med_ref, mad_ref, mask_ref, turned, place, facts, inverse, quota):
    drifts = mask_ref.shape[0]
    coarse = place.shape[0]
    keys = PER * drifts
    wide = jnp.broadcast_to(om_ref[...], (coarse, coarse))
    down, across = iota((coarse, coarse), 0), iota((coarse, coarse), 1)
    tall = jnp.sum(jnp.where(down == across, wide, 0), axis=1, keepdims=True)
    rank_tall = jnp.sum(one(wide < tall, jnp.int32), axis=1, keepdims=True)
    rank_wide = jnp.sum(one(tall < wide, F32), axis=0, keepdims=True)
    found = jnp.sum(jnp.where(rank_tall == across, down, 0), axis=0, keepdims=True)
    inverse[...] = jnp.minimum(found, coarse - 1)
    sort = one(rank_wide == down.astype(F32))

    turned[...] = mask_ref[...].astype(F32).T
    marks = jnp.concatenate([turned[pl.ds(b, coarse, stride=PER), :] for b in range(PER)], axis=1)
    marks = jnp.dot(sort, marks.astype(BF16), preferred_element_type=F32)
    rank_a = iota((keys, keys), 0)
    rank_b = iota((keys, keys), 1)
    rank_a = (rank_a % drifts) * PER + rank_a // drifts
    rank_b = (rank_b % drifts) * PER + rank_b // drifts
    before = jnp.dot(marks.astype(BF16), one(rank_a < rank_b), preferred_element_type=F32)
    count = jnp.sum(marks, axis=1, keepdims=True)
    ahead = (down // quota == across // quota) & (across < down)
    offset = jnp.dot(
        one(ahead),
        jnp.broadcast_to(count, (coarse, keys)).astype(BF16),
        preferred_element_type=F32,
    )
    place[...] = jnp.where(marks > 0, offset + before, -1.0)

    med = med_ref[...]
    own = jnp.concatenate(
        [
            (med // 256).astype(F32),
            (med % 256).astype(F32),
            mad_ref[...].astype(F32),
            (om_ref[...] % coarse).astype(F32),
            jnp.zeros((4, coarse), F32),
        ],
        axis=0,
    ).astype(BF16)
    own = lax.dot_general(own, sort, NT, preferred_element_type=F32)
    facts[0:1, :] = BIN_STEP * (own[0:1] * 256.0 + own[1:2])
    facts[1:3, :] = own[2:4]


def send_kernel(
    freq_count, quota, om_ref, med_ref, mad_ref, med_s, mad_s, mask_ref, spec_ref,
    rows_in, tags_in, mom_in,
    buf, turned, place, facts, inverse, inverse_s, sums, rows_out, tags_out, mom_out,
    load_sem, inv_sem, own_sem, row_send, row_recv, tag_send, tag_recv, mom_send, mom_recv,
):
    me = lax.axis_index("freq")
    half = lax.axis_index("sub")
    drifts = mask_ref.shape[0]
    coarse = place.shape[0]
    keys = PER * drifts

    def load(c):
        at = pl.multiple_of(c * COARSE_WIDTH, COARSE_WIDTH)
        return pltpu.make_async_copy(
            spec_ref.at[:, pl.ds(at, COARSE_WIDTH)], buf.at[c], load_sem.at[c]
        )

    lax.fori_loop(0, coarse, lambda c, _: load(c).start(), None, unroll=4)

    others = [(d, s) for d in range(freq_count) for s in range(2) if d or s]

    def peer(d, s):
        return {"freq": lax.rem(me + d, freq_count), "sub": lax.rem(half + s, 2)}

    barrier = pltpu.get_barrier_semaphore()
    for d, s in others:
        pl.semaphore_signal(barrier, inc=1, device_id=peer(d, s), device_id_type=MESH)

    plan(om_ref, med_ref, mad_ref, mask_ref, turned, place, facts, inverse, quota)
    to_scalars = pltpu.make_async_copy(inverse, inverse_s, inv_sem.at[0])
    to_scalars.start()
    to_scalars.wait()
    lax.fori_loop(0, coarse, lambda c, _: load(c).wait(), None, unroll=4)
    pl.semaphore_wait(barrier, len(others))

    spot = iota((CAP, keys), 0).astype(F32).astype(BF16)
    lane = iota((8, keys), 1)
    row = iota((8, keys), 0)
    order = ((lane % drifts) * PER + lane // drifts).astype(F32)
    half_f = half.astype(F32)

    def channel(q, j):
        c = inverse_s[0, q]
        center = BIN_STEP * med_s[c].astype(F32)
        spread = MAD_WIDTH * BIN_STEP * mad_s[c].astype(F32)
        low, high = center - spread, center + spread
        total = [jnp.zeros((8, BLOCK), F32) for _ in range(3)]
        tiles = []
        for b in range(PER):
            tile = buf[c, :, b * BLOCK : (b + 1) * BLOCK]
            tiles.append(tile)
            x = tile.astype(F32)
            inside = (x >= low) & (x <= high)
            kept = jnp.where(inside, x - center, 0.0)
            for i, v in enumerate((one(inside, F32), kept, kept * kept)):
                for r in range(0, drifts, 8):
                    total[i] = total[i] + v[r : r + 8]
        for i in range(3):
            sums[i, pl.ds(q, 1), :] = jnp.sum(total[i], axis=0, keepdims=True)
        line = jnp.broadcast_to(place[pl.ds(q, 1), :], (16, keys)).astype(BF16)
        pick = one(jnp.concatenate([line] * (CAP // 16), axis=0) == spot)
        tag = jnp.where(
            row == 0,
            order,
            jnp.where(row == 1, j.astype(F32), jnp.where(row == 2, 1.0, jnp.where(row == 3, half_f, 0.0))),
        ).astype(BF16)
        return (
            jnp.dot(pick, jnp.concatenate(tiles, axis=0), preferred_element_type=F32),
            lax.dot_general(tag, pick, NT, preferred_element_type=F32),
        )

    def move(src, dst, send, recv, d, s):
        return pltpu.make_async_remote_copy(
            src_ref=src, dst_ref=dst, send_sem=send, recv_sem=recv,
            device_id=peer(d, s), device_id_type=MESH,
        )

    def hits(d):
        o = lax.rem(me + d, freq_count)
        return (
            move(rows_out.at[o], rows_in.at[me], row_send.at[d], row_recv.at[d], d, 0),
            move(tags_out.at[o], tags_in.at[me], tag_send.at[d], tag_recv.at[d], d, 0),
        )

    group = min(quota, UNROLL)

    def owner(step, _):
        d = lax.rem(step + 1, freq_count)
        o = lax.rem(me + d, freq_count)

        def some(p, carry):
            rows, tags = carry
            for u in range(group):
                j = p * group + u
                more = channel(o * quota + j, j)
                rows, tags = rows + more[0], tags + more[1]
            return rows, tags

        rows, tags = lax.fori_loop(
            0, quota // group, some, (jnp.zeros((CAP, BLOCK), F32), jnp.zeros((8, CAP), F32))
        )
        rows_out[o] = rows.astype(BF16)
        tags_out[o] = tags

        @pl.when(step < freq_count - 1)
        def _():
            for copy in hits(d):
                copy.start()

        return 0

    lax.fori_loop(0, freq_count, owner, 0)

    flat = [jnp.sum(sums[i].T, axis=0, keepdims=True) for i in range(3)]
    info = jnp.where(half == 0, facts[0:3, :], 0.0)
    tile = jnp.concatenate(flat + [info, jnp.zeros((2, coarse), F32)], axis=0)
    parts = jnp.concatenate(split3(tile), axis=0).astype(BF16)
    down, across = iota((coarse, coarse), 0), iota((coarse, coarse), 1)
    for o in range(freq_count):
        shift = one((down - o * quota == across - me * quota) & (across // quota == me))
        got = jnp.dot(parts, shift, preferred_element_type=F32)
        mom_out[o] = got[0:8] + got[8:16] + got[16:24]

    own = (
        pltpu.make_async_copy(rows_out.at[me], rows_in.at[me], own_sem.at[0]),
        pltpu.make_async_copy(tags_out.at[me], tags_in.at[me], own_sem.at[1]),
        pltpu.make_async_copy(mom_out.at[me], mom_in.at[me, half], own_sem.at[2]),
    )
    for copy in own:
        copy.start()
    moments = [
        move(
            mom_out.at[lax.rem(me + d, freq_count)], mom_in.at[me, half],
            mom_send.at[2 * d + s], mom_recv.at[2 * d + s], d, s,
        )
        for d, s in others
    ]
    for copy in moments:
        copy.start()
    for copy in own:
        copy.wait()
    for d in range(1, freq_count):
        for copy in hits(d):
            copy.wait()
    for copy in moments:
        copy.wait()


def list_kernel(freq_count, quota, drift_total, rows_ref, tags_ref, mom_ref, snr_ref, keys_ref, excess_ref):
    coarse = mom_ref.shape[3]
    width = freq_count * CAP
    table = jnp.zeros((8, coarse), F32)
    for f in range(freq_count):
        table = table + (mom_ref[f, 0] + mom_ref[f, 1])
    floor_count = jnp.maximum(table[0:1], 1.0)
    mean_level = table[3:4] + table[1:2] / floor_count
    mad_sigma = MAD_SCALE * BIN_STEP * table[4:5]
    sigma = jnp.sqrt(0.5 * table[2:3] / floor_count + 0.5 * mad_sigma * mad_sigma)
    lookup = jnp.concatenate(
        split3(mean_level) + split3(1.0 / sigma) + [table[5:6], jnp.zeros((1, coarse), F32)], axis=0
    ).astype(BF16)

    begin = jnp.zeros((1, 1), F32)
    dst, digits = [], []
    lanes = iota((1, CAP), 1).astype(F32)
    row = iota((8, CAP), 0)
    for f in range(freq_count):
        tags = tags_ref[f]
        live = tags[2:3] > 0.5
        dst.append(jnp.where(live, begin + lanes, -1.0))
        digits.append(tags + jnp.where(row == 1, float(f * quota), 0.0))
        begin = begin + jnp.sum(one(live, F32), axis=1, keepdims=True)
    dst = jnp.concatenate(dst, axis=1)
    digits = jnp.concatenate(digits, axis=1).astype(BF16)
    spot = iota((CAP, width), 0).astype(F32).astype(BF16)
    arrived = rows_ref[...].reshape(width, BLOCK)
    index = iota((coarse, CAP), 0).astype(F32)

    def block(k, at):
        local = jnp.clip(dst - k * float(CAP), -1.0, float(CAP))
        line = jnp.broadcast_to(local, (16, width)).astype(BF16)
        pick = one(jnp.concatenate([line] * (CAP // 16), axis=0) == spot)
        raw = jnp.dot(pick, arrived, preferred_element_type=F32)
        got = lax.dot_general(digits, pick, NT, preferred_element_type=F32)
        filled = got[2:3] > 0.5
        hot = one((index == got[1:2]) & filled)
        vals = jnp.dot(lookup, hot, preferred_element_type=F32)
        level = vals[0:1] + vals[1:2] + vals[2:3]
        scale = vals[3:4] + vals[4:5] + vals[5:6]
        cols = jnp.concatenate([level, scale, jnp.zeros((6, CAP), F32)], axis=0).T
        snr = ((raw - cols[:, 0:1]) * cols[:, 1:2]).astype(BF16)
        snr_ref[pl.ds(at, CAP), :] = snr
        key = vals[6:7] * float(drift_total * PER) + got[3:4] * float(drift_total // 2 * PER) + got[0:1]
        keys_ref[:, pl.ds(at, CAP)] = jnp.where(filled, key, -1.0).astype(jnp.int32)
        over = jnp.maximum(snr.astype(F32) - THRESH, 0.0)
        excess_ref[:, pl.ds(at, CAP)] = jnp.sum(over.T, axis=0, keepdims=True)

    if freq_count <= 8:
        for k in range(freq_count):
            block(float(k), k * CAP)
    else:

        @pl.loop(0, freq_count)
        def _(k):
            block(k.astype(F32), pl.multiple_of(k * CAP, CAP))


def per_device(spectrum, hit_mask, owner_map, median_bin, mad_bin):
    drift_dev = spectrum.shape[0]
    coarse = owner_map.shape[0]
    freq_count = lax.axis_size("freq")
    drift_total = drift_dev * lax.axis_size("sub")
    width = freq_count * CAP
    quota = coarse // freq_count
    smem = pl.BlockSpec(memory_space=pltpu.SMEM)
    vmem = pl.BlockSpec(memory_space=pltpu.VMEM)
    anyw = pl.BlockSpec(memory_space=pl.ANY)
    dma = pltpu.SemaphoreType.DMA
    rows, tags, moments = pl.pallas_call(
        functools.partial(send_kernel, freq_count, quota),
        out_shape=(
            jax.ShapeDtypeStruct((freq_count, CAP, BLOCK), BF16),
            jax.ShapeDtypeStruct((freq_count, 8, CAP), F32),
            jax.ShapeDtypeStruct((freq_count, 2, 8, coarse), F32),
        ),
        in_specs=[vmem, vmem, vmem, smem, smem, vmem, anyw],
        out_specs=(OUT_SPEC,) * 3,
        scratch_shapes=[
            pltpu.VMEM((coarse, drift_dev, COARSE_WIDTH), BF16),
            pltpu.VMEM((coarse * PER, drift_dev), F32),
            pltpu.VMEM((coarse, PER * drift_dev), F32),
            pltpu.VMEM((8, coarse), F32),
            pltpu.VMEM((1, coarse), jnp.int32),
            pltpu.SMEM((1, coarse), jnp.int32),
            pltpu.VMEM((3, coarse, BLOCK), F32),
            pltpu.VMEM((freq_count, CAP, BLOCK), BF16),
            pltpu.VMEM((freq_count, 8, CAP), F32),
            pltpu.VMEM((freq_count, 8, coarse), F32),
            dma((coarse,)),
            dma((1,)),
            dma((3,)),
            dma((freq_count,)),
            dma((freq_count,)),
            dma((freq_count,)),
            dma((freq_count,)),
            dma((2 * freq_count,)),
            dma((2 * freq_count,)),
        ],
        compiler_params=pltpu.CompilerParams(collective_id=0, has_side_effects=True),
        name="moments_pick_send",
    )(
        owner_map.reshape(1, coarse),
        median_bin.reshape(1, coarse),
        mad_bin.reshape(1, coarse),
        median_bin,
        mad_bin,
        hit_mask,
        spectrum,
    )
    snr, keys, excess = pl.pallas_call(
        functools.partial(list_kernel, freq_count, quota, drift_total),
        out_shape=(
            jax.ShapeDtypeStruct((width, BLOCK), BF16),
            jax.ShapeDtypeStruct((1, width), jnp.int32),
            jax.ShapeDtypeStruct((1, width), F32),
        ),
        in_specs=[vmem] * 3,
        out_specs=(vmem,) * 3,
        name="normalize_and_list",
    )(rows, tags, moments)
    return (
        snr.reshape(1, 1, width, BLOCK),
        keys.reshape(1, 1, width),
        excess.reshape(1, 1, width),
    )


def solution(mesh):
    placed = (
        P("sub", ("beam", "freq")),
        P("sub", ("beam", "freq")),
        P(("beam", "freq")),
        P(("beam", "freq")),
        P(("beam", "freq")),
    )
    return jax.shard_map(
        per_device,
        mesh=mesh,
        in_specs=placed,
        out_specs=(
            P("freq", "sub", "beam", None),
            P("freq", "sub", "beam"),
            P("freq", "sub", "beam"),
        ),
        check_vma=False,
    )
```

```python
import functools

import jax
import jax.numpy as jnp
from jax import lax
from jax.experimental import pallas as pl
from jax.experimental.pallas import tpu as pltpu
from jax.sharding import PartitionSpec as P

COARSE_WIDTH = 1024
BLOCK = 128
CAP = 128
PER = COARSE_WIDTH // BLOCK

BIN_STEP = 0.0625
MAD_WIDTH = 5.0
MAD_SCALE = 1.4826
THRESH = 3.0

F32 = jnp.float32
BF16 = jnp.bfloat16
MESH = pl.DeviceIdType.MESH
NT = (((1,), (1,)), ((), ()))
UNROLL = 16
OUT_SPEC = pl.BlockSpec(memory_space=pl.ANY)


def iota(shape, dim):
    return lax.broadcasted_iota(jnp.int32, shape, dim)


def one(mask, dtype=BF16):
    return jnp.where(mask, jnp.ones((), dtype), jnp.zeros((), dtype))


def split3(v):
    a = v.astype(BF16).astype(F32)
    b = (v - a).astype(BF16).astype(F32)
    return [a, b, v - a - b]


def plan(om_ref, med_ref, mad_ref, mask_ref, turned, place, mom_out, inverse, freq_count, quota, me, half):
    drifts = mask_ref.shape[0]
    coarse = place.shape[0]
    keys = PER * drifts
    wide = jnp.broadcast_to(om_ref[...], (coarse, coarse))
    down, across = iota((coarse, coarse), 0), iota((coarse, coarse), 1)
    tall = jnp.sum(jnp.where(down == across, wide, 0), axis=1, keepdims=True)
    rank_tall = jnp.sum(one(wide < tall, jnp.int32), axis=1, keepdims=True)
    rank_wide = jnp.sum(one(tall < wide, F32), axis=0, keepdims=True)
    found = jnp.sum(jnp.where(rank_tall == across, down, 0), axis=0, keepdims=True)
    inverse[...] = jnp.minimum(found, coarse - 1)
    sort = one(rank_wide == down.astype(F32))

    turned[...] = mask_ref[...].astype(F32).T
    marks = jnp.concatenate([turned[pl.ds(b, coarse, stride=PER), :] for b in range(PER)], axis=1)
    marks = jnp.dot(sort, marks.astype(BF16), preferred_element_type=F32)
    rank_a = iota((keys, keys), 0)
    rank_b = iota((keys, keys), 1)
    rank_a = (rank_a % drifts) * PER + rank_a // drifts
    rank_b = (rank_b % drifts) * PER + rank_b // drifts
    before = jnp.dot(marks.astype(BF16), one(rank_a < rank_b), preferred_element_type=F32)
    count = jnp.sum(marks, axis=1, keepdims=True)
    ahead = (down // quota == across // quota) & (across < down)
    offset = jnp.dot(
        one(ahead),
        jnp.broadcast_to(count, (coarse, keys)).astype(BF16),
        preferred_element_type=F32,
    )
    place[...] = jnp.where(marks > 0, offset + before, -1.0)

    med = med_ref[...]
    own = jnp.concatenate(
        [
            (med // 256).astype(F32),
            (med % 256).astype(F32),
            mad_ref[...].astype(F32),
            (om_ref[...] % coarse).astype(F32),
            jnp.zeros((4, coarse), F32),
        ],
        axis=0,
    ).astype(BF16)
    own = lax.dot_general(own, sort, NT, preferred_element_type=F32)
    for o in range(freq_count):
        shift = one((down - o * quota == across - me * quota) & (across // quota == me))
        got = jnp.dot(own.astype(BF16), shift, preferred_element_type=F32)
        center = BIN_STEP * (got[0:1] * 256.0 + got[1:2])
        info = jnp.concatenate([jnp.zeros((3, coarse), F32), center, got[2:4], jnp.zeros((2, coarse), F32)], axis=0)
        mom_out[o] = jnp.where(half == 0, info, 0.0)


def send_kernel(
    freq_count, quota, om_ref, med_ref, mad_ref, med_s, mad_s, mask_ref, spec_ref,
    rows_in, tags_in, mom_in,
    buf, turned, place, inverse, inverse_s, sums, rows_out, tags_out, mom_out,
    load_sem, inv_sem, own_sem, row_send, row_recv, tag_send, tag_recv, mom_send, mom_recv,
):
    me = lax.axis_index("freq")
    half = lax.axis_index("sub")
    drifts = mask_ref.shape[0]
    coarse = place.shape[0]
    keys = PER * drifts

    def load(c):
        at = pl.multiple_of(c * COARSE_WIDTH, COARSE_WIDTH)
        return pltpu.make_async_copy(
            spec_ref.at[:, pl.ds(at, COARSE_WIDTH)], buf.at[c], load_sem.at[0]
        )

    lax.fori_loop(0, coarse, lambda c, _: load(c).start(), None, unroll=4)

    others = [(d, s) for d in range(freq_count) for s in range(2) if d or s]

    def peer(d, s):
        return {"freq": lax.rem(me + d, freq_count), "sub": lax.rem(half + s, 2)}

    barrier = pltpu.get_barrier_semaphore()
    for d, s in others:
        pl.semaphore_signal(barrier, inc=1, device_id=peer(d, s), device_id_type=MESH)

    plan(om_ref, med_ref, mad_ref, mask_ref, turned, place, mom_out, inverse, freq_count, quota, me, half)
    to_scalars = pltpu.make_async_copy(inverse, inverse_s, inv_sem.at[0])
    to_scalars.start()
    to_scalars.wait()
    pltpu.make_async_copy(buf, buf, load_sem.at[0]).wait()
    pl.semaphore_wait(barrier, len(others))

    spot = iota((CAP, keys), 0).astype(F32).astype(BF16)
    lane = iota((8, keys), 1)
    row = iota((8, keys), 0)
    order = ((lane % drifts) * PER + lane // drifts).astype(F32)
    half_f = half.astype(F32)

    def channel(q, j):
        c = inverse_s[0, q]
        center = BIN_STEP * med_s[c].astype(F32)
        spread = MAD_WIDTH * BIN_STEP * mad_s[c].astype(F32)
        low, high = center - spread, center + spread
        total = [jnp.zeros((8, BLOCK), F32) for _ in range(3)]
        tiles = []
        for b in range(PER):
            tile = buf[c, :, b * BLOCK : (b + 1) * BLOCK]
            tiles.append(tile)
            x = tile.astype(F32)
            inside = (x >= low) & (x <= high)
            kept = jnp.where(inside, x - center, 0.0)
            for i, v in enumerate((one(inside, F32), kept, kept * kept)):
                for r in range(0, drifts, 8):
                    total[i] = total[i] + v[r : r + 8]
        for i in range(3):
            sums[i, pl.ds(q, 1), :] = jnp.sum(total[i], axis=0, keepdims=True)
        line = jnp.broadcast_to(place[pl.ds(q, 1), :], (16, keys)).astype(BF16)
        pick = one(jnp.concatenate([line] * (CAP // 16), axis=0) == spot)
        tag = jnp.where(
            row == 0,
            order,
            jnp.where(row == 1, j.astype(F32), jnp.where(row == 2, 1.0, jnp.where(row == 3, half_f, 0.0))),
        ).astype(BF16)
        return (
            jnp.dot(pick, jnp.concatenate(tiles, axis=0), preferred_element_type=F32),
            lax.dot_general(tag, pick, NT, preferred_element_type=F32),
        )

    def move(src, dst, send, recv, d, s):
        return pltpu.make_async_remote_copy(
            src_ref=src, dst_ref=dst, send_sem=send, recv_sem=recv,
            device_id=peer(d, s), device_id_type=MESH,
        )

    def hits(d):
        o = lax.rem(me + d, freq_count)
        return (
            move(rows_out.at[o], rows_in.at[me], row_send.at[d], row_recv.at[d], d, 0),
            move(tags_out.at[o], tags_in.at[me], tag_send.at[d], tag_recv.at[d], d, 0),
        )

    def level(d, s):
        return move(
            mom_out.at[lax.rem(me + d, freq_count)], mom_in.at[me, half],
            mom_send.at[2 * d + s], mom_recv.at[2 * d + s], d, s,
        )

    group = min(quota, UNROLL)

    def owner(step, _):
        d = lax.rem(step + 1, freq_count)
        o = lax.rem(me + d, freq_count)

        def some(p, carry):
            rows, tags = carry
            for u in range(group):
                j = p * group + u
                more = channel(o * quota + j, j)
                rows, tags = rows + more[0], tags + more[1]
            return rows, tags

        rows, tags = lax.fori_loop(
            0, quota // group, some, (jnp.zeros((CAP, BLOCK), F32), jnp.zeros((8, CAP), F32))
        )
        rows_out[o] = rows.astype(BF16)
        tags_out[o] = tags
        sub = iota((quota, coarse), 0)
        mine = iota((quota, coarse), 1) == me * quota + sub
        flat = []
        for i in range(3):
            each = jnp.sum(sums[i, pl.ds(o * quota, quota), :], axis=1, keepdims=True)
            flat.append(jnp.sum(jnp.where(mine, each, 0.0), axis=0, keepdims=True))
        mom_out[o] += jnp.concatenate(flat + [jnp.zeros((5, coarse), F32)], axis=0)

        @pl.when(step < freq_count - 1)
        def _():
            for copy in hits(d) + (level(d, 0), level(d, 1)):
                copy.start()

        return 0

    lax.fori_loop(0, freq_count, owner, 0)

    level(0, 1).start()
    own = (
        pltpu.make_async_copy(rows_out.at[me], rows_in.at[me], own_sem.at[0]),
        pltpu.make_async_copy(tags_out.at[me], tags_in.at[me], own_sem.at[1]),
        pltpu.make_async_copy(mom_out.at[me], mom_in.at[me, half], own_sem.at[2]),
    )
    for copy in own:
        copy.start()
    for copy in own:
        copy.wait()
    for d in range(1, freq_count):
        for copy in hits(d):
            copy.wait()
    for d, s in others:
        level(d, s).wait()


def list_kernel(freq_count, quota, drift_total, rows_ref, tags_ref, mom_ref, snr_ref, keys_ref, excess_ref):
    coarse = mom_ref.shape[3]
    width = freq_count * CAP
    table = jnp.zeros((8, coarse), F32)
    for f in range(freq_count):
        table = table + (mom_ref[f, 0] + mom_ref[f, 1])
    floor_count = jnp.maximum(table[0:1], 1.0)
    mean_level = table[3:4] + table[1:2] / floor_count
    mad_sigma = MAD_SCALE * BIN_STEP * table[4:5]
    sigma = jnp.sqrt(0.5 * table[2:3] / floor_count + 0.5 * mad_sigma * mad_sigma)
    lookup = jnp.concatenate(
        split3(mean_level) + split3(1.0 / sigma) + [table[5:6], jnp.zeros((1, coarse), F32)], axis=0
    ).astype(BF16)

    begin = jnp.zeros((1, 1), F32)
    dst, digits = [], []
    lanes = iota((1, CAP), 1).astype(F32)
    row = iota((8, CAP), 0)
    for f in range(freq_count):
        tags = tags_ref[f]
        live = tags[2:3] > 0.5
        dst.append(jnp.where(live, begin + lanes, -1.0))
        digits.append(tags + jnp.where(row == 1, float(f * quota), 0.0))
        begin = begin + jnp.sum(one(live, F32), axis=1, keepdims=True)
    dst = jnp.concatenate(dst, axis=1)
    digits = jnp.concatenate(digits, axis=1).astype(BF16)
    spot = iota((CAP, width), 0).astype(F32).astype(BF16)
    arrived = rows_ref[...].reshape(width, BLOCK)
    index = iota((coarse, CAP), 0).astype(F32)

    def block(k, at):
        local = jnp.clip(dst - k * float(CAP), -1.0, float(CAP))
        line = jnp.broadcast_to(local, (16, width)).astype(BF16)
        pick = one(jnp.concatenate([line] * (CAP // 16), axis=0) == spot)
        raw = jnp.dot(pick, arrived, preferred_element_type=F32)
        got = lax.dot_general(digits, pick, NT, preferred_element_type=F32)
        filled = got[2:3] > 0.5
        hot = one((index == got[1:2]) & filled)
        vals = jnp.dot(lookup, hot, preferred_element_type=F32)
        level = vals[0:1] + vals[1:2] + vals[2:3]
        scale = vals[3:4] + vals[4:5] + vals[5:6]
        cols = jnp.concatenate([level, scale, jnp.zeros((6, CAP), F32)], axis=0).T
        snr = ((raw - cols[:, 0:1]) * cols[:, 1:2]).astype(BF16)
        snr_ref[pl.ds(at, CAP), :] = snr
        key = vals[6:7] * float(drift_total * PER) + got[3:4] * float(drift_total // 2 * PER) + got[0:1]
        keys_ref[:, pl.ds(at, CAP)] = jnp.where(filled, key, -1.0).astype(jnp.int32)
        over = jnp.maximum(snr.astype(F32) - THRESH, 0.0)
        excess_ref[:, pl.ds(at, CAP)] = jnp.sum(over.T, axis=0, keepdims=True)

    if freq_count <= 8:
        for k in range(freq_count):
            block(float(k), k * CAP)
    else:

        @pl.loop(0, freq_count)
        def _(k):
            block(k.astype(F32), pl.multiple_of(k * CAP, CAP))


def per_device(spectrum, hit_mask, owner_map, median_bin, mad_bin):
    drift_dev = spectrum.shape[0]
    coarse = owner_map.shape[0]
    freq_count = lax.axis_size("freq")
    drift_total = drift_dev * lax.axis_size("sub")
    width = freq_count * CAP
    quota = coarse // freq_count
    smem = pl.BlockSpec(memory_space=pltpu.SMEM)
    vmem = pl.BlockSpec(memory_space=pltpu.VMEM)
    anyw = pl.BlockSpec(memory_space=pl.ANY)
    dma = pltpu.SemaphoreType.DMA
    rows, tags, moments = pl.pallas_call(
        functools.partial(send_kernel, freq_count, quota),
        out_shape=(
            jax.ShapeDtypeStruct((freq_count, CAP, BLOCK), BF16),
            jax.ShapeDtypeStruct((freq_count, 8, CAP), F32),
            jax.ShapeDtypeStruct((freq_count, 2, 8, coarse), F32),
        ),
        in_specs=[vmem, vmem, vmem, smem, smem, vmem, anyw],
        out_specs=(OUT_SPEC,) * 3,
        scratch_shapes=[
            pltpu.VMEM((coarse, drift_dev, COARSE_WIDTH), BF16),
            pltpu.VMEM((coarse * PER, drift_dev), F32),
            pltpu.VMEM((coarse, PER * drift_dev), F32),
            pltpu.VMEM((1, coarse), jnp.int32),
            pltpu.SMEM((1, coarse), jnp.int32),
            pltpu.VMEM((3, coarse, BLOCK), F32),
            pltpu.VMEM((freq_count, CAP, BLOCK), BF16),
            pltpu.VMEM((freq_count, 8, CAP), F32),
            pltpu.VMEM((freq_count, 8, coarse), F32),
            dma((1,)),
            dma((1,)),
            dma((3,)),
            dma((freq_count,)),
            dma((freq_count,)),
            dma((freq_count,)),
            dma((freq_count,)),
            dma((2 * freq_count,)),
            dma((2 * freq_count,)),
        ],
        compiler_params=pltpu.CompilerParams(collective_id=0, has_side_effects=True),
        name="moments_pick_send",
    )(
        owner_map.reshape(1, coarse),
        median_bin.reshape(1, coarse),
        mad_bin.reshape(1, coarse),
        median_bin,
        mad_bin,
        hit_mask,
        spectrum,
    )
    snr, keys, excess = pl.pallas_call(
        functools.partial(list_kernel, freq_count, quota, drift_total),
        out_shape=(
            jax.ShapeDtypeStruct((width, BLOCK), BF16),
            jax.ShapeDtypeStruct((1, width), jnp.int32),
            jax.ShapeDtypeStruct((1, width), F32),
        ),
        in_specs=[vmem] * 3,
        out_specs=(vmem,) * 3,
        name="normalize_and_list",
    )(rows, tags, moments)
    return (
        snr.reshape(1, 1, width, BLOCK),
        keys.reshape(1, 1, width),
        excess.reshape(1, 1, width),
    )


def solution(mesh):
    placed = (
        P("sub", ("beam", "freq")),
        P("sub", ("beam", "freq")),
        P(("beam", "freq")),
        P(("beam", "freq")),
        P(("beam", "freq")),
    )
    return jax.shard_map(
        per_device,
        mesh=mesh,
        in_specs=placed,
        out_specs=(
            P("freq", "sub", "beam", None),
            P("freq", "sub", "beam"),
            P("freq", "sub", "beam"),
        ),
        check_vma=False,
    )
```
